32 devices in a mesh: dp: 2 (over x), inner: 4 (over z), vocab: 4 (over y, core).
Axes of the slice: x: 2, y: 2, z: 4, core: 2. Of those that a mesh axis runs over, the one named last changes fastest.
Arguments:
- hidden: bfloat16 [1024, 1536], P('dp'), parts along dimension 0
- w_head: bfloat16 [1536, 151936], P(None, ('vocab', 'inner'))
- inv_temp: float32 [1024], P('dp'), parts along dimension 0
- target_id: int32 [1024], P('dp'), parts along dimension 0
Outputs:
- output 1: float32 [1024, 151936], P('dp', ('vocab', 'inner')), parts along dimension 0
- output 2: float32 [1024], P('dp'), parts along dimension 0
There are 2 independent parts. The reference program is written for one: setup_inputs(seed, part) draws one part's arguments, and reference() takes and returns one part's arrays. A program takes and returns all parts, laid end to end along the dimension named above; an argument that names none is the same for every part.
All inputs are finite; a program needn't handle non-finite values.
Results may differ from the reference program's by a relative error of at most 0.001.
Values are sent between devices in bfloat16 or wider.
A program may use at most 1 GiB of HBM per device.

```python
import jax
import jax.numpy as jnp

B = 512
D = 1536
V = 151936


def setup_inputs(seed: int = 0, part: int = 0) -> dict:
    base_key = jax.random.key(seed)
    rows_key, weight_key = jax.random.split(base_key)
    part_key = jax.random.fold_in(rows_key, part)
    noise_key, shift_key, slope_key, temp_key, target_key = jax.random.split(part_key, 5)
    dim_even = (jnp.arange(D) % 2) == 0
    shift_amp = jax.random.uniform(shift_key, (B, 1), jnp.float32, 0.0, 2.0)
    slope_amp = jax.random.uniform(slope_key, (B, 1), jnp.float32, 0.8, 1.2)
    row_mean = jnp.where(dim_even[None, :], shift_amp, slope_amp)
    hidden = jax.random.normal(noise_key, (B, D), jnp.float32) + row_mean
    inv_temp = jax.random.uniform(temp_key, (B,), jnp.float32, 0.6, 1.4)
    token_rank = jnp.log1p(jnp.arange(V).astype(jnp.float32))
    col_mean = jnp.where(dim_even[:, None], 50.0, -token_rank[None, :]) * (2.0 / D)
    w_head = jax.random.normal(weight_key, (D, V), jnp.float32) * (D ** -0.5) + col_mean
    low_key, high_key = jax.random.split(target_key)
    any_id = jax.random.randint(low_key, (B,), 0, V)
    late_id = jax.random.randint(high_key, (B,), V // 2, V)
    target_id = jnp.where(jnp.arange(B) % 4 == 0, any_id, late_id).astype(jnp.int32)
    return {'hidden': hidden.astype(jnp.bfloat16), 'w_head': w_head.astype(jnp.bfloat16), 'inv_temp': inv_temp, 'target_id': target_id}


def reference(hidden, w_head, inv_temp, target_id):
    logits = jnp.dot(hidden, w_head, preferred_element_type=jnp.float32) * inv_temp[:, None]
    row_max = jnp.max(logits, axis=1, keepdims=True)
    exp_shift = jnp.exp(logits - row_max)
    row_sum = jnp.sum(exp_shift, axis=1, keepdims=True)
    cdf_table = jnp.cumsum(exp_shift / row_sum, axis=1)
    col_ids = jnp.arange(V)
    cdf_target = jnp.sum(jnp.where(col_ids[None, :] == target_id[:, None], cdf_table, 0.0), axis=1)
    return cdf_table, cdf_target
```

```python
import functools

import jax
import jax.numpy as jnp
from jax import lax
from jax.experimental import pallas as pl
from jax.experimental.pallas import tpu as pltpu
from jax.sharding import PartitionSpec as P

VOCAB_AXES = ('vocab', 'inner')
F32 = jnp.float32
LANES = 128
ROWS = 432
W_SLOTS = 4
OUT_SLOTS = 3


def _row(block, k):
    return block[k:k + 1, :]


def _head_kernel(n_vocab, n_inner, invt_hbm, tgt_hbm, hid_hbm, w_hbm, c_ref, off_ref, fac_ref, pre_ref, glob_ref,
                 invt_ref, tgt_ref, hid, hid_t, wbuf, z, mx, tot, tq, recv, hsem, wsem, send_sem, recv_sem):
    vocab, depth = w_hbm.shape
    batch = hid.shape[0]
    n_l = batch // LANES
    n_t = pl.cdiv(vocab, ROWS)
    last_rows = vocab - (n_t - 1) * ROWS
    n_dev = n_vocab * n_inner
    my_v, my_i = lax.axis_index('vocab'), lax.axis_index('inner')
    me = my_v * n_inner + my_i
    shard_start = me * vocab

    def peer(k):
        p = lax.rem(me + k, n_dev)
        return p, {'vocab': p // n_inner, 'inner': lax.rem(p, n_inner)}

    barrier = pltpu.get_barrier_semaphore()
    for k in range(1, n_dev):
        pl.semaphore_signal(barrier, inc=1, device_id=peer(k)[1], device_id_type=pl.DeviceIdType.MESH)

    def w_copy(t, slot, rows):
        return pltpu.make_async_copy(
            w_hbm.at[pl.ds(t * ROWS, rows), :], wbuf.at[slot, pl.ds(0, rows), :], wsem.at[slot])

    small = [pltpu.make_async_copy(src, dst, hsem.at[k]) for k, (src, dst) in enumerate(
        [(hid_hbm, hid), (invt_hbm, invt_ref), (tgt_hbm, tgt_ref)])]
    for copy in small:
        copy.start()
    for t in range(W_SLOTS - 1):
        w_copy(t, t, ROWS).start()
    for copy in small:
        copy.wait()
    hid_t[...] = hid[...].T

    invt = [_row(invt_ref[...], l) for l in range(n_l)]
    sub = lax.broadcasted_iota(jnp.int32, (8, LANES), 0)

    def matmul(t, slot, zslot, rows):
        zt = jnp.dot(wbuf[slot, :rows, :], hid_t[...], preferred_element_type=F32)
        for l in range(n_l):
            zl = zt[:, l * LANES:(l + 1) * LANES] * invt[l]
            z[zslot, l, :rows, :] = zl
            mx[t, l:l + 1, :] = jnp.max(zl, axis=0, keepdims=True)

    def prefix(t, zslot, rows):
        group = rows // 8
        first = shard_start + t * ROWS
        peak = [jnp.broadcast_to(mx[t, l:l + 1, :], (8, LANES)) for l in range(n_l)]
        rel = [tgt_ref[l:l + 1, :] - first - sub * group for l in range(n_l)]
        acc = [jnp.zeros((8, LANES), F32) for _ in range(n_l)]
        at_target = [jnp.zeros((8, LANES), F32) for _ in range(n_l)]
        for j in range(group):
            for l in range(n_l):
                e = jnp.exp(z.at[zslot, l][pl.ds(j, 8, stride=group), :] - peak[l])
                acc[l] = acc[l] + e
                c_ref[pl.ds(t * ROWS + 8 * j, 8), l * LANES:(l + 1) * LANES] = acc[l]
                at_target[l] = jnp.where(rel[l] == j, acc[l], at_target[l])
        for l in range(n_l):
            x = acc[l]
            for s in (1, 2, 4):
                x = x + jnp.where(sub >= s, pltpu.roll(x, s, 0), 0.0)
            excl = jnp.where(sub >= 1, pltpu.roll(x, 1, 0), 0.0)
            off_ref[t, l * 8:(l + 1) * 8, :] = excl
            tot[t, l:l + 1, :] = x[7:8, :]
            inside = (rel[l] >= 0) & (rel[l] < group)
            tq[t, l:l + 1, :] = jnp.sum(jnp.where(inside, at_target[l] + excl, 0.0), axis=0, keepdims=True)

    w_copy(0, 0, ROWS).wait()
    w_copy(W_SLOTS - 1, W_SLOTS - 1, ROWS).start()
    matmul(0, 0, 0, ROWS)

    def step(t, _):
        slot = lax.rem(t, W_SLOTS)
        w_copy(t, slot, ROWS).wait()
        ahead = t + W_SLOTS - 1
        ahead_slot = lax.rem(ahead, W_SLOTS)

        @pl.when(ahead < n_t - 1)
        def _():
            w_copy(ahead, ahead_slot, ROWS).start()

        @pl.when(ahead == n_t - 1)
        def _():
            w_copy(n_t - 1, ahead_slot, last_rows).start()

        zslot = lax.rem(t, 2)
        matmul(t, slot, zslot, ROWS)
        prefix(t - 1, 1 - zslot, ROWS)
        return 0

    lax.fori_loop(1, n_t - 1, step, 0)
    t_last = n_t - 1
    w_copy(t_last, t_last % W_SLOTS, last_rows).wait()
    matmul(t_last, t_last % W_SLOTS, t_last % 2, last_rows)
    prefix(t_last - 1, (t_last - 1) % 2, ROWS)
    prefix(t_last, t_last % 2, last_rows)

    tgt = tgt_ref[...]
    m_loc = jnp.max(mx[...], axis=0)
    run = jnp.zeros((n_l, LANES), F32)
    q_loc = jnp.zeros((n_l, LANES), F32)
    for t in range(n_t):
        fac = jnp.exp(mx[t] - m_loc)
        fac_ref[t] = fac
        pre_ref[t] = run
        lo = shard_start + t * ROWS
        hi = shard_start + min((t + 1) * ROWS, vocab)
        q_loc = q_loc + jnp.where((tgt >= lo) & (tgt < hi), tq[t] * fac + run, 0.0)
        run = run + tot[t] * fac
    recv[me, 0:n_l, :] = m_loc
    recv[me, n_l:2 * n_l, :] = run
    recv[me, 2 * n_l:3 * n_l, :] = q_loc

    pl.semaphore_wait(barrier, n_dev - 1)

    def stat_copy(k):
        return pltpu.make_async_remote_copy(
            src_ref=recv.at[me], dst_ref=recv.at[me], send_sem=send_sem.at[k], recv_sem=recv_sem.at[me],
            device_id=peer(k)[1], device_id_type=pl.DeviceIdType.MESH)

    for k in range(1, n_dev):
        stat_copy(k).start()
    for k in range(1, n_dev):
        p, where = peer(k)
        pltpu.make_async_remote_copy(
            src_ref=recv.at[p], dst_ref=recv.at[p], send_sem=send_sem.at[k], recv_sem=recv_sem.at[p],
            device_id=where, device_id_type=pl.DeviceIdType.MESH).wait_recv()

    m_all = recv[0, 0:n_l, :]
    for p in range(1, n_dev):
        m_all = jnp.maximum(m_all, recv[p, 0:n_l, :])
    total = jnp.zeros((n_l, LANES), F32)
    before = jnp.zeros((n_l, LANES), F32)
    up_to = jnp.zeros((n_l, LANES), F32)
    for p in range(n_dev):
        f = jnp.exp(recv[p, 0:n_l, :] - m_all)
        s = recv[p, n_l:2 * n_l, :] * f
        total = total + s
        before = before + jnp.where(p < me, s, 0.0)
        up_to = up_to + jnp.where(tgt >= (p + 1) * vocab, s, recv[p, 2 * n_l:3 * n_l, :] * f)
    glob_ref[0] = jnp.exp(m_loc - m_all) / total
    glob_ref[1] = before / total
    glob_ref[2] = up_to / total
    for k in range(1, n_dev):
        stat_copy(k).wait_send()


def _write_kernel(c_ref, off_ref, fac_ref, pre_ref, glob_ref, out_hbm, tgt_out, stage, sem):
    vocab, batch = out_hbm.shape
    n_l = batch // LANES
    n_t = pl.cdiv(vocab, ROWS)
    last_rows = vocab - (n_t - 1) * ROWS
    gain = glob_ref[0]
    base = glob_ref[1]
    tgt_out[...] = glob_ref[2]

    def out_copies(t, slot, rows):
        return [pltpu.make_async_copy(
            stage.at[slot, l, pl.ds(0, rows), :],
            out_hbm.at[pl.ds(t * ROWS, rows), l * LANES:(l + 1) * LANES], sem.at[slot, l]) for l in range(n_l)]

    def fill(t, slot, rows):
        group = rows // 8
        a_all = fac_ref[t] * gain
        d_all = pre_ref[t] * gain + base
        for l in range(n_l):
            a = jnp.broadcast_to(_row(a_all, l), (8, LANES))
            b = off_ref[t, l * 8:(l + 1) * 8, :] * a + _row(d_all, l)
            for j in range(group):
                c = c_ref[pl.ds(t * ROWS + 8 * j, 8), l * LANES:(l + 1) * LANES]
                stage.at[slot, l][pl.ds(j, 8, stride=group), :] = c * a + b

    def step(t, _):
        slot = lax.rem(t, OUT_SLOTS)

        @pl.when(t >= OUT_SLOTS)
        def _():
            for copy in out_copies(t - OUT_SLOTS, slot, ROWS):
                copy.wait()

        fill(t, slot, ROWS)
        for copy in out_copies(t, slot, ROWS):
            copy.start()
        return 0

    lax.fori_loop(0, n_t - 1, step, 0)
    t_last = n_t - 1
    for copy in out_copies(t_last - OUT_SLOTS, t_last % OUT_SLOTS, ROWS):
        copy.wait()
    fill(t_last, t_last % OUT_SLOTS, last_rows)
    for copy in out_copies(t_last, t_last % OUT_SLOTS, last_rows):
        copy.start()
    for t in range(n_t - OUT_SLOTS, n_t):
        for copy in out_copies(t, t % OUT_SLOTS, last_rows if t == t_last else ROWS):
            copy.wait()


def solution(mesh):
    n_vocab, n_inner = mesh.shape['vocab'], mesh.shape['inner']
    n_dev = n_vocab * n_inner
    vmem = pl.BlockSpec(memory_space=pltpu.VMEM)
    hbm = pl.BlockSpec(memory_space=pltpu.HBM)

    def local_step(hidden, w_shard, inv_temp, target_id):
        batch, depth = hidden.shape
        vocab = w_shard.shape[1]
        n_l = batch // LANES
        n_t = pl.cdiv(vocab, ROWS)
        mid_shapes = [(vocab, batch), (n_t, 8 * n_l, LANES), (n_t, n_l, LANES), (n_t, n_l, LANES), (3, n_l, LANES)]
        mids = pl.pallas_call(
            functools.partial(_head_kernel, n_vocab, n_inner),
            out_shape=[pltpu.VMEM(s, F32) for s in mid_shapes],
            in_specs=[hbm] * 4,
            out_specs=[vmem] * 5,
            scratch_shapes=[
                pltpu.VMEM((n_l, LANES), F32),
                pltpu.VMEM((n_l, LANES), jnp.int32),
                pltpu.VMEM((batch, depth), jnp.bfloat16),
                pltpu.VMEM((depth, batch), jnp.bfloat16),
                pltpu.VMEM((W_SLOTS, ROWS, depth), jnp.bfloat16),
                pltpu.VMEM((2, n_l, ROWS, LANES), F32),
                pltpu.VMEM((n_t, n_l, LANES), F32),
                pltpu.VMEM((n_t, n_l, LANES), F32),
                pltpu.VMEM((n_t, n_l, LANES), F32),
                pltpu.VMEM((n_dev, 3 * n_l, LANES), F32),
                pltpu.SemaphoreType.DMA((3,)),
                pltpu.SemaphoreType.DMA((W_SLOTS,)),
                pltpu.SemaphoreType.DMA((n_dev,)),
                pltpu.SemaphoreType.DMA((n_dev,)),
            ],
            compiler_params=pltpu.CompilerParams(
                collective_id=0, has_side_effects=True, vmem_limit_bytes=24 * 2 ** 20),
            name='head',
        )(inv_temp.reshape(n_l, LANES), target_id.reshape(n_l, LANES), hidden, w_shard.T)
        table_t, at_target = pl.pallas_call(
            _write_kernel,
            out_shape=[jax.ShapeDtypeStruct((vocab, batch), F32), jax.ShapeDtypeStruct((n_l, LANES), F32)],
            in_specs=[vmem] * 5,
            out_specs=[hbm, vmem],
            scratch_shapes=[
                pltpu.VMEM((OUT_SLOTS, n_l, ROWS, LANES), F32),
                pltpu.SemaphoreType.DMA((OUT_SLOTS, n_l)),
            ],
            compiler_params=pltpu.CompilerParams(vmem_limit_bytes=8 * 2 ** 20),
            name='table',
        )(*mids)
        return table_t.T, at_target.reshape(batch)

    return jax.shard_map(local_step, mesh=mesh, in_specs=(P('dp', None), P(None, VOCAB_AXES), P('dp'), P('dp')),
                         out_specs=(P('dp', VOCAB_AXES), P('dp')), check_vma=False)
```
